32 devices in a mesh: grp: 2 (over y), wide: 16 (over z, x, core).
Axes of the slice: x: 2, y: 2, z: 4, core: 2. Of those that a mesh axis runs over, the one named last changes fastest.
Arguments:
- activations: bfloat16 [2, 1024, 4096], P('grp', 'wide'), parts along dimension 0, may hold values from -6 to 6
- output_grads: bfloat16 [2, 1024, 4096], P('grp', None, 'wide'), parts along dimension 0, may hold values from -0.1875 to 0.1875
- token_ids: int32 [2, 1024], P('grp'), parts along dimension 0, may hold values from 0 to 128255, as said below
- row_signs: int32 [4096], replicated, may hold values from -1 to 1, as said below
- column_signs: int32 [4096], replicated, may hold values from -1 to 1, as said below
- kept_blocks: int32 [8192], P('wide'), may hold values from 0 to 131071, as said below
- queries: bfloat16 [256, 1048576], P(None, 'wide'), may hold values from -0.0078125 to 0.0078125
Outputs:
- sketches: bfloat16 [2, 1048576], P('grp', 'wide'), parts along dimension 0
- scores: float32 [256, 2], P('wide', 'grp'), parts along dimension 1
The draws below stay inside these ranges and needn't reach their ends.
There are 2 independent parts, one for each index of `grp`. The reference program is written for one: setup_inputs(seed, part) draws one part's arguments, and reference() takes and returns one part's arrays. A program takes and returns all parts, laid end to end along the dimension named above; an argument that names none is the same for every part. Nothing has to cross between parts.
Inputs may be any that keep to these rules, and one draw needn't show every extreme that they name: `token_ids`: id 0 marks padding. Each sequence ends with one run of one or more padding ids, and 512 or more of its ids are 1 or more. `row_signs`: every entry is +1 or -1. `column_signs`: every entry is +1 or -1. `kept_blocks`: A block number b names column b // 32 and rows (b % 32) * 128 up to (b % 32 + 1) * 128 - 1 of a sequence's projected matrix. For every d, entries d * 512 up to (d + 1) * 512 - 1 are distinct and name columns d * 256 up to (d + 1) * 256 - 1.
All inputs are finite; a program needn't handle non-finite values.
Results may differ from the reference program's by a relative error of at most 0.006.
Values may be sent and summed in bfloat16 or wider, within the bound.
No kernel may reach another device: no remote copies, remote signals or barrier semaphores. Data moves between devices by JAX's collectives and lax.ppermute only.
A program may use at most 256 MiB of HBM per device.

```python
import jax
import jax.numpy as jnp
from jax import lax

D = 4096
ROWBLK = 128
K_BLOCKS = 8192
VOCAB = 128256
SEQS = 1
LEN = 1024
NQ = 256
COLS_DEV = 256
NBLK = 32
KEPT_DEV = 512
SKETCH = 1048576
N_WIDE = 16


def draw_token_ids(key, part):
    length_key = jax.random.fold_in(key, 13)
    token_key = jax.random.fold_in(key, 17)
    lengths = jax.random.randint(length_key, (SEQS,), LEN // 2, LEN)
    drawn = jax.random.randint(token_key, (SEQS, LEN), 1, VOCAB)
    positions = jnp.arange(LEN, dtype=jnp.int32)
    sequence_index = jnp.arange(SEQS, dtype=jnp.int32)
    topmost = (positions[None, :] == 0) & (sequence_index[:, None] == 0)
    drawn = jnp.where(topmost, VOCAB - 1, drawn)
    return jnp.where(positions[None, :] < lengths[:, None], drawn, 0).astype(jnp.int32)


def draw_row_signs(key, part):
    drawn = jax.random.randint(jax.random.fold_in(key, 11), (D,), 0, 2)
    return (2 * drawn - 1).astype(jnp.int32)


def draw_column_signs(key, part):
    drawn = jax.random.randint(jax.random.fold_in(key, 12), (D,), 0, 2)
    return (2 * drawn - 1).astype(jnp.int32)


def draw_kept_blocks(key, part):
    slab_keys = jax.random.split(jax.random.fold_in(key, 14), N_WIDE)
    per_slab = COLS_DEV * NBLK
    slab_index = jnp.arange(N_WIDE, dtype=jnp.int32)

    def one_slab(slab_key, slab_number):
        order = jax.random.permutation(slab_key, per_slab).astype(jnp.int32)
        target = jnp.where(slab_number == N_WIDE - 1, per_slab - 1, 0).astype(jnp.int32)
        places = jnp.arange(per_slab, dtype=jnp.int32)
        where_target = jnp.sum(jnp.where(order == target, places, 0)).astype(jnp.int32)
        first_value = order[0]
        swapped = jnp.where(places == 0, target, jnp.where(places == where_target, first_value, order))
        return swapped[:KEPT_DEV]
    chosen = jax.vmap(one_slab)(slab_keys, slab_index).astype(jnp.int32)
    offsets = slab_index[:, None] * per_slab
    return (chosen + offsets).reshape(K_BLOCKS).astype(jnp.int32)


def strengthened(entries, rng, source, target, shards_of, factor):
    def block_of(dim):
        return (jnp.arange(entries.shape[dim]) // (entries.shape[dim] // shards_of)).reshape((-1,) + (1,) * (entries.ndim - 1 - dim))

    first = jax.random.permutation(rng, shards_of)[block_of(target)]
    second = (block_of(target) + shards_of // 2) % shards_of
    return jnp.where((block_of(source) == first) | (block_of(source) == second), factor * entries, entries)


def shard_levels(rng, dims, cuts, least, top_value):
    def one(dim, blocks):
        heights = jax.random.uniform(jax.random.fold_in(jax.random.fold_in(rng, 6), dim), (blocks,), jnp.float32, least / len(cuts), top_value / len(cuts))
        return jnp.repeat(jnp.exp(heights), dims[dim] // blocks).reshape((-1,) + (1,) * (len(dims) - dim - 1))

    factor_of = one(*cuts[0])
    for cut in cuts[1:]:
        factor_of = factor_of * one(*cut)
    return factor_of


def normal_values(stream_key, dims, spread, reach, cuts=(), held_as=jnp.bfloat16):
    array = jax.random.normal(stream_key, dims, jnp.float32) * spread
    if len(cuts) > 0:
        array = shard_levels(stream_key, dims, cuts, -0.22, 0.18) * array
    return jnp.clip(array, min=-reach, max=reach).astype(held_as)


def gaussian_with(key, extent, scale, limit, pieces, heavy, kind=jnp.bfloat16):
    entries = scale * jax.random.normal(key, extent, jnp.float32)
    if pieces:
        entries = entries * shard_levels(key, extent, pieces, -0.22, 0.18)
    return jnp.clip(strengthened(entries, jax.random.fold_in(key, 3), *heavy), -limit, limit).astype(kind)


def setup_inputs(seed: int = 0, part: int = 0) -> dict:
    keys = jax.random.split(jax.random.key(seed), 8)
    part_splits = jax.random.split(jax.random.fold_in(keys[7], part), 8)
    activations = normal_values(part_splits[0], (SEQS, LEN, D), 1.0, 6.0, ((1, 16),))
    output_grads = normal_values(part_splits[1], (SEQS, LEN, D), LEN ** -0.5, 0.1875, ((2, 16),))
    token_ids = draw_token_ids(jax.random.fold_in(jax.random.fold_in(keys[7], part), 71), part)
    row_signs = draw_row_signs(jax.random.fold_in(keys[7], 71), part)
    column_signs = draw_column_signs(jax.random.fold_in(keys[7], 71), part)
    kept_blocks = draw_kept_blocks(jax.random.fold_in(keys[7], 71), part)
    queries = gaussian_with(keys[6], (NQ, SKETCH), SKETCH ** -0.5, 0.0078125, ((1, 16),), (1, 0, 16, 2.0))
    return dict(activations=activations, output_grads=output_grads, token_ids=token_ids, row_signs=row_signs, column_signs=column_signs, kept_blocks=kept_blocks, queries=queries)


def sign_table(bit_count):
    length = 2 ** bit_count
    indices = jnp.arange(length, dtype=jnp.int32)
    common = jnp.bitwise_and(indices[:, None], indices[None, :])
    parity = jnp.zeros((length, length), jnp.int32)
    for position in range(bit_count):
        parity = parity + jnp.bitwise_and(jnp.right_shift(common, position), 1)
    signs = 1 - 2 * jnp.bitwise_and(parity, 1)
    return (signs.astype(jnp.float32) * (length ** -0.5)).astype(jnp.bfloat16)


def hadamard_table(order_size):
    total_bits = order_size.bit_length() - 1
    low_bits = total_bits // 2
    high_table = sign_table(total_bits - low_bits)
    low_table = sign_table(low_bits)
    high_table, low_table = lax.optimization_barrier((high_table, low_table))
    return (high_table[:, None, :, None] * low_table[None, :, None, :]).reshape(order_size, order_size)


def reference(activations, output_grads, token_ids, row_signs, column_signs, kept_blocks, queries):
    hadamard = hadamard_table(D)
    hadamard_wide = hadamard.astype(jnp.float32)
    row_blocks = D // ROWBLK
    column_sign = column_signs.astype(jnp.bfloat16)
    row_sign = row_signs.astype(jnp.bfloat16)

    def one_sequence(sequence_inputs):
        activation_rows, gradient_rows, token_row = sequence_inputs
        weight = (token_row != 0).astype(jnp.bfloat16)
        signed_inputs = (activation_rows * column_sign[None, :]).astype(jnp.float32)
        turned = jnp.dot(signed_inputs, hadamard_wide,
                         preferred_element_type=jnp.float32).astype(jnp.bfloat16)
        weighted = (gradient_rows * weight[:, None]).astype(jnp.float32)
        half_turned = jnp.dot(weighted.T, turned.astype(jnp.float32),
                              preferred_element_type=jnp.float32).astype(jnp.bfloat16)
        signed = (half_turned * row_sign[:, None]).astype(jnp.float32)
        projected = jnp.dot(hadamard_wide, signed, preferred_element_type=jnp.float32)
        block_rows = projected.T.reshape(D * row_blocks, ROWBLK)
        picked = jnp.take(block_rows, kept_blocks.astype(jnp.int32), axis=0)
        return picked.reshape(K_BLOCKS * ROWBLK).astype(jnp.bfloat16)

    sketches = lax.map(one_sequence, (activations, output_grads, token_ids))
    scores = jnp.dot(queries.astype(jnp.float32), sketches.astype(jnp.float32).T,
                     preferred_element_type=jnp.float32)
    return sketches, scores
```

```python
import functools

import jax
import jax.numpy as jnp
from jax import lax
from jax.experimental import pallas as pl
from jax.experimental.pallas import tpu as pltpu
from jax.sharding import PartitionSpec as P

ROWBLK = 128
AXIS = "wide"
VMEM = pltpu.VMEM


def sign_table(bit_count):
    length = 2**bit_count
    indices = jnp.arange(length, dtype=jnp.int32)
    common = jnp.bitwise_and(indices[:, None], indices[None, :])
    parity = jnp.zeros((length, length), jnp.int32)
    for position in range(bit_count):
        parity = parity + jnp.bitwise_and(jnp.right_shift(common, position), 1)
    signs = 1 - 2 * jnp.bitwise_and(parity, 1)
    return (signs.astype(jnp.float32) * length ** (-0.5)).astype(jnp.bfloat16)


def hadamard_table(order_size):
    total_bits = order_size.bit_length() - 1
    low_bits = total_bits // 2
    high_table = sign_table(total_bits - low_bits)
    low_table = sign_table(low_bits)
    high_table, low_table = lax.optimization_barrier((high_table, low_table))
    return (high_table[:, None, :, None] * low_table[None, :, None, :]).reshape(
        order_size, order_size
    )


def general_form(
    activations, output_grads, token_ids, row_signs, column_signs, kept_blocks, queries
):
    model_width = column_signs.shape[0]
    hadamard = hadamard_table(model_width)
    row_blocks = model_width // ROWBLK
    column_sign = column_signs.astype(jnp.bfloat16)
    row_sign = row_signs.astype(jnp.bfloat16)
    weight = (token_ids != 0).astype(jnp.bfloat16)
    columns_dev = output_grads.shape[2]
    device = lax.axis_index(AXIS)
    local_blocks = kept_blocks - device * (columns_dev * row_blocks)
    turned = jnp.einsum(
        "stj,jk->stk",
        activations * column_sign[None, None, :],
        hadamard,
        preferred_element_type=jnp.float32,
    ).astype(jnp.bfloat16)
    columns = lax.all_to_all(turned, AXIS, split_axis=2, concat_axis=1, tiled=True)
    weighted = columns * weight[:, :, None]
    half_turned = jnp.einsum(
        "stc,sti->sci",
        weighted,
        lax.all_gather(output_grads, AXIS, axis=2, tiled=True),
        preferred_element_type=jnp.float32,
    ).astype(jnp.bfloat16)
    signed = half_turned * row_sign[None, None, :]
    projected = jnp.einsum("scj,ji->sci", signed, hadamard, preferred_element_type=jnp.float32)
    items = projected.shape[0]
    block_rows = projected.reshape(items, projected.shape[1] * row_blocks, ROWBLK)
    picked = jnp.take(block_rows, local_blocks, axis=1)
    sketches = picked.reshape(items, picked.shape[1] * ROWBLK).astype(jnp.bfloat16)
    scores = lax.psum_scatter(
        jnp.einsum("qc,sc->qs", queries, sketches, preferred_element_type=jnp.float32),
        AXIS,
        scatter_dimension=0,
        tiled=True,
    )
    return (sketches, scores)


def sign_of(a, b):
    p = a & b
    for shift in (16, 8, 4, 2, 1):
        p = p ^ (p >> shift)
    return (1 - 2 * (p & 1)).astype(jnp.float32)


def signs_matrix(size):
    p = lax.broadcasted_iota(jnp.int32, (size, size), 0) & lax.broadcasted_iota(
        jnp.int32, (size, size), 1
    )
    shift = 1
    while shift * 2 < size:
        shift *= 2
    while shift:
        p = p ^ (p >> shift)
        shift //= 2
    return (1 - 2 * (p & 1)).astype(jnp.float32).astype(jnp.bfloat16)


def butterfly(values):
    values = list(values)
    span = 1
    while span < len(values):
        for i in range(len(values)):
            if not i & span:
                a, b = values[i], values[i | span]
                values[i], values[i | span] = a + b, a - b
        span *= 2
    return values


def turn_kernel(n, inner, scale, act_ref, sign_ref, *rest):
    out_refs, part = rest[:inner], rest[inner]
    me = lax.axis_index(AXIS)
    rows, width = act_ref.shape[1], act_ref.shape[2] // n
    table = signs_matrix(width)
    for hi in range(n):
        cols = pl.ds(hi * width, width)
        s = sign_ref[:, cols].astype(jnp.float32) * sign_of(me, hi)
        a = act_ref[0, :, cols] * s.astype(jnp.bfloat16)
        part[hi] = jnp.dot(a, table, preferred_element_type=jnp.float32)
    for r in range(0, rows, 16):
        for c in range(0, width, 128):
            at = (pl.ds(r, 16), pl.ds(c, 128))
            got = butterfly([part[(hi, *at)] for hi in range(n)])
            for kappa in range(n):
                out_refs[kappa % inner][(kappa // inner, *at)] = (got[kappa] * scale).astype(
                    jnp.bfloat16
                )


def spin_kernel(n, scale, *refs):
    pieces, (row_ref, spun, part) = refs[:n], refs[n:]
    me = lax.axis_index(AXIS)
    tokens, width = pieces[0].shape
    table = signs_matrix(width)
    for kappa in range(n):
        at = pl.multiple_of((me ^ kappa) * width, width)
        s = row_ref[:, pl.ds(at, width)].astype(jnp.float32).astype(jnp.bfloat16)
        part[kappa] = jnp.dot(pieces[kappa][...] * s, table, preferred_element_type=jnp.float32)
    factors = [sign_of(me, hi) * scale for hi in range(n)]

    def spin(step, carry):
        r = pl.multiple_of(step * 16, 16)
        for c in range(0, width, 128):
            at = (pl.ds(r, 16), pl.ds(c, 128))
            got = butterfly([part[(kappa, *at)] for kappa in range(n)])
            for hi in range(n):
                spun[(hi, *at)] = (got[hi] * factors[hi]).astype(jnp.bfloat16)
        return carry

    lax.fori_loop(0, tokens // 16, spin, 0)


def pick_kernel(inner, owners, *refs):
    turned = refs[:inner]
    rows = refs[inner : inner + len(owners)]
    spun, token_ref = refs[inner + len(owners) : inner + len(owners) + 2]
    outs = refs[inner + len(owners) + 2 : inner + 2 * len(owners) + 2]
    cols_in, prod, chosen = refs[inner + 2 * len(owners) + 2 :]
    me = lax.axis_index(AXIS)
    n, tokens, width = spun.shape
    unit = (
        lax.broadcasted_iota(jnp.int32, (width, width), 0)
        == lax.broadcasted_iota(jnp.int32, (width, width), 1)
    ).astype(jnp.float32).astype(jnp.bfloat16)
    first = pl.multiple_of((me // inner) * tokens, tokens)
    weight = (token_ref[:, pl.ds(first, tokens)] != 0).astype(jnp.float32)
    per = tokens // inner
    sub = width // ROWBLK
    count = rows[0].shape[0]
    for at_owner, k in enumerate(owners):
        for j in range(inner):
            to = pl.multiple_of(((me % inner) ^ j) * per, per)
            cols_in[pl.ds(to, per), :] = turned[j][k]
        xt = lax.dot_general(
            unit, cols_in[...], (((1,), (1,)), ((), ())), preferred_element_type=jnp.float32
        )
        xt = (xt * weight).astype(jnp.bfloat16)
        for hi in range(n):
            got = jnp.dot(xt, spun[hi], preferred_element_type=jnp.float32)
            for h in range(sub):
                prod[pl.ds((hi * sub + h) * width, width), :] = got[:, h * ROWBLK : (h + 1) * ROWBLK]

        def choose(step, carry, at_owner=at_owner):
            for u in range(16):
                at = step * 16 + u
                row = rows[at_owner][at]
                chosen[pl.ds(at, 1), :] = prod[pl.ds(row, 1), :]
            return carry

        lax.fori_loop(0, count // 16, choose, 0)
        outs[at_owner][...] = chosen[...].astype(jnp.bfloat16)


def score_kernel(outer, offset, last, *refs):
    parts, query_ref = refs[:outer], refs[outer]
    refs = refs[outer + 1 :]
    before, refs = (refs[0], refs[1:]) if offset else (None, refs)
    sketch_ref, score_ref, wide, acc = refs
    total = parts[0][...].astype(jnp.float32)
    for p in parts[1:]:
        total = total + p[...].astype(jnp.float32)
    sketch = total.astype(jnp.bfloat16)
    sketch_ref[...] = sketch
    wide[...] = sketch.astype(jnp.float32)
    rows, queries = sketch.shape[0], acc.shape[0]
    acc[...] = jnp.zeros_like(acc) if before is None else before[...]

    def add(step, carry):
        for q in range(0, queries, 64):
            run = acc[pl.ds(q, 64), :]
            for k in range(16):
                row = step * 16 + k
                at = pl.multiple_of(offset * ROWBLK + row * ROWBLK, ROWBLK)
                run = run + query_ref[pl.ds(q, 64), pl.ds(at, ROWBLK)].astype(
                    jnp.float32
                ) * jnp.broadcast_to(wide[pl.ds(row, 1), :], (64, ROWBLK))
            acc[pl.ds(q, 64), :] = run
        return carry

    lax.fori_loop(0, rows // 16, add, 0)
    if last:
        score_ref[...] = lax.dot_general(
            jnp.ones((8, ROWBLK), jnp.float32),
            acc[...],
            (((1,), (1,)), ((), ())),
            precision=lax.Precision.HIGHEST,
            preferred_element_type=jnp.float32,
        )
    else:
        score_ref[...] = acc[...]


def far_first(outer):
    return sorted(range(outer), key=lambda k: (k < outer // 2, k == 0, k))


def shuffled(n, x, mask):
    return lax.ppermute(x, AXIS, [(i, i ^ mask) for i in range(n)])


def split_form(
    n, inner, activations, output_grads, token_ids, row_signs, column_signs, kept_blocks, queries
):
    outer = n // inner
    width = output_grads.shape[2]
    total = output_grads.shape[1]
    per = total // n
    tokens = per * inner
    model_width = column_signs.shape[0]
    count = kept_blocks.shape[0]
    scale = float(model_width) ** -0.5
    me = lax.axis_index(AXIS)
    z = me // inner
    move = functools.partial(shuffled, n)
    whole = pl.BlockSpec(memory_space=VMEM)
    smem = pl.BlockSpec(memory_space=pltpu.SMEM)
    small = pltpu.CompilerParams(vmem_limit_bytes=20 * 2**20)

    def cost(flops):
        return pl.CostEstimate(flops=flops, bytes_accessed=flops // 256, transcendentals=0)


    grads = output_grads[0]
    mine = {}
    for k in far_first(outer):
        piece = lax.dynamic_slice_in_dim(grads, (z ^ k) * tokens, tokens, 0)
        mine[k] = move(piece, k * inner) if k else piece
    turned = pl.pallas_call(
        functools.partial(turn_kernel, n, inner, scale),
        out_shape=[jax.ShapeDtypeStruct((outer, per, width), jnp.bfloat16)] * inner,
        in_specs=[whole, whole],
        out_specs=[whole] * inner,
        scratch_shapes=[VMEM((n, per, width), jnp.float32)],
        compiler_params=small,
        cost_estimate=cost(2 * per * model_width * width),
        name="turn",
    )(activations, column_signs[None, :])
    turned = [move(t, j) if j else t for j, t in enumerate(turned)]
    blocks = model_width // ROWBLK
    block_rows = (kept_blocks % blocks) * width + (kept_blocks // blocks) % width
    picks = [move(block_rows, k * inner) if k else block_rows for k in range(outer)]
    pieces = {}
    for k in [0] + list(reversed(far_first(outer)))[1:]:
        have = {0: mine[k]}
        bit = inner // 2
        while bit:
            for j in list(have):
                have[j | bit] = move(have[j], bit)
            bit //= 2
        for j in range(inner):
            pieces[k * inner + j] = have[j]

    spun = pl.pallas_call(
        functools.partial(spin_kernel, n, scale),
        out_shape=jax.ShapeDtypeStruct((n, tokens, width), jnp.bfloat16),
        in_specs=[whole] * (n + 1),
        out_specs=whole,
        scratch_shapes=[VMEM((n, tokens, width), jnp.float32)],
        compiler_params=small,
        cost_estimate=cost(2 * tokens * model_width * width),
        name="spin",
    )(*[pieces[kappa] for kappa in range(n)], row_signs[None, :])

    chosen = {}
    for owners in (far_first(outer)[: outer // 2], far_first(outer)[outer // 2 :]):
        got = pl.pallas_call(
            functools.partial(pick_kernel, inner, owners),
            out_shape=[jax.ShapeDtypeStruct((count, ROWBLK), jnp.bfloat16)] * len(owners),
            in_specs=[whole] * inner + [smem] * len(owners) + [whole, whole],
            out_specs=[whole] * len(owners),
            scratch_shapes=[
                VMEM((tokens, width), jnp.bfloat16),
                VMEM((n * width * width // ROWBLK, ROWBLK), jnp.float32),
                VMEM((count, ROWBLK), jnp.float32),
            ],
            compiler_params=small,
            cost_estimate=cost(2 * tokens * model_width * width * len(owners)),
            name="pick",
        )(*turned, *[picks[k] for k in owners], spun, token_ids)
        chosen.update(zip(owners, got))
    parts = [move(chosen[k], k * inner) if k else chosen[k] for k in range(outer)]

    nq = queries.shape[0]
    sketch, score = pl.pallas_call(
        functools.partial(score_kernel, outer, 0, True),
        out_shape=[
            jax.ShapeDtypeStruct((count, ROWBLK), jnp.bfloat16),
            jax.ShapeDtypeStruct((8, nq), jnp.float32),
        ],
        in_specs=[whole] * (outer + 1),
        out_specs=[whole, whole],
        scratch_shapes=[VMEM((count, ROWBLK), jnp.float32), VMEM((nq, ROWBLK), jnp.float32)],
        compiler_params=small,
        cost_estimate=cost(2 * nq * count * ROWBLK),
        name="score",
    )(*parts, queries)

    run = score[0].reshape(n, nq // n)
    bit = 1
    while bit < n:
        pair = run.reshape(-1, 2, nq // n) if bit == 1 else run.reshape(run.shape[0] // 2, 2, nq // n)
        side = (me // bit) % 2
        run = lax.dynamic_index_in_dim(pair, side, 1, False) + move(
            lax.dynamic_index_in_dim(pair, 1 - side, 1, False), bit
        )
        bit *= 2
    return sketch.reshape(1, count * ROWBLK), run.reshape(nq // n, 1)


def solution(mesh):
    n = mesh.shape[AXIS]
    bits = n.bit_length() - 1
    inner = 2 ** (bits // 2)

    def per_device(activations, output_grads, *rest):
        items, per, _ = activations.shape
        width = output_grads.shape[2]
        fits = items == 1 and n == 2**bits and width % ROWBLK == 0 and per % 16 == 0
        fits = fits and width == per * inner
        if fits:
            return split_form(n, inner, activations, output_grads, *rest)
        return general_form(activations, output_grads, *rest)

    placed = (
        P("grp", AXIS, None),
        P("grp", None, AXIS),
        P("grp", None),
        P(),
        P(),
        P(AXIS),
        P(None, AXIS),
    )
    return jax.shard_map(
        per_device,
        mesh=mesh,
        in_specs=placed,
        out_specs=(P("grp", AXIS), P(AXIS, "grp")),
        check_vma=False,
    )
```
